32 devices in a mesh: member: 2 (over x), mp: 16 (over z, y, core).
Axes of the slice: x: 2, y: 2, z: 4, core: 2. Of those that a mesh axis runs over, the one named last changes fastest.
Arguments:
- nodes: bfloat16 [2048, 4096], P(('member', 'mp')), parts along dimension 0, may hold values from -6 to 6
- norm_gain: float32 [4096], replicated, may hold values from 0.1 to 1.9
- w_in: bfloat16 [4096, 16384], P(None, 'mp'), may hold values from -0.09375 to 0.09375
- b_in: float32 [16384], P('mp'), may hold values from -3 to 3
- w_out: bfloat16 [16384, 4096], P('mp'), may hold values from -0.046875 to 0.046875
- b_out: float32 [4096], replicated, may hold values from -3 to 3
Outputs:
- updated: bfloat16 [2048, 4096], P(('member', 'mp')), parts along dimension 0
The draws below stay inside these ranges and needn't reach their ends.
There are 2 independent parts, one for each index of `member`. The reference program is written for one: setup_inputs(seed, part) draws one part's arguments, and reference() takes and returns one part's arrays. A program takes and returns all parts, laid end to end along the dimension named above; an argument that names none is the same for every part. Nothing has to cross between parts.
All inputs are finite; a program needn't handle non-finite values.
Results may differ from the reference program's by a relative error of at most 0.015.
Values may be sent and summed in bfloat16 or wider, within the bound.
No kernel may reach another device: no remote copies, remote signals or barrier semaphores. Data moves between devices by JAX's collectives and lax.ppermute only.
A program may use at most 128 MiB of HBM per device.

```python
import jax
import jax.numpy as jnp
from jax import lax

D = 4096
FF = 16384
ROWS = 1024
N_MP = 16


def levels(key, extent, pieces, low, high):
    loudness = 1.0
    for dim, blocks in pieces:
        draws = jax.random.uniform(jax.random.fold_in(jax.random.fold_in(key, 6), dim), (blocks,), jnp.float32, low / len(pieces), high / len(pieces))
        loudness = loudness * jnp.repeat(jnp.exp(draws), extent[dim] // blocks).reshape((-1,) + (1,) * (len(extent) - 1 - dim))
    return loudness


def gaussian(key, shape, deviation, limit, cuts=(), kind=jnp.bfloat16):
    drawn = deviation * jax.random.normal(key, shape, jnp.float32)
    if cuts:
        drawn = drawn * levels(key, shape, cuts, -0.22, 0.18)
    return jnp.clip(drawn, -limit, limit).astype(kind)


def setup_inputs(seed: int = 0, part: int = 0) -> dict:
    key_list = jax.random.split(jax.random.key(seed), 7)
    own_keys = jax.random.split(jax.random.fold_in(key_list[6], part), 7)
    return {
        "nodes": gaussian(own_keys[0], (ROWS, D), 1.0, 6.0, ((0, 16),)),
        "norm_gain": jnp.clip(1.0 + 0.18 * jax.random.normal(key_list[1], (D,), jnp.float32), 0.1, 1.9),
        "w_in": gaussian(key_list[2], (D, FF), D ** -0.5, 0.09375, ((1, 16),)),
        "b_in": gaussian(key_list[3], (FF,), 0.5, 3.0, ((0, 16),), jnp.float32),
        "w_out": gaussian(key_list[4], (FF, D), FF ** -0.5, 0.046875, ((0, 16),)),
        "b_out": gaussian(key_list[5], (D,), 0.5, 3.0, (), jnp.float32),
    }


def reference(nodes, norm_gain, w_in, b_in, w_out, b_out):
    values = nodes.astype(jnp.float32)
    mean = lax.optimization_barrier(jnp.mean(values, axis=1, keepdims=True))
    var = lax.optimization_barrier(jnp.mean((values - mean) ** 2, axis=1, keepdims=True))
    normed = ((values - mean) / jnp.sqrt(var + 1e-05) * norm_gain).astype(jnp.bfloat16)
    pre = jnp.dot(normed, w_in, preferred_element_type=jnp.float32) + b_in
    hidden = jax.nn.gelu(pre, approximate=True).astype(jnp.bfloat16)
    width = FF // N_MP

    def add_share(index, total):
        start = (index * width).astype(jnp.int32)
        left = lax.dynamic_slice_in_dim(hidden, start, width, 1)
        right = lax.dynamic_slice_in_dim(w_out, start, width, 0)
        share = jnp.dot(left, right, preferred_element_type=jnp.float32).astype(jnp.bfloat16)
        return total + share.astype(jnp.float32)
    mlp_out = lax.fori_loop(jnp.int32(0), jnp.int32(N_MP), add_share, jnp.zeros((nodes.shape[0], nodes.shape[1]), jnp.float32))
    return (values + mlp_out + b_out).astype(jnp.bfloat16)
```

```python
import jax
import jax.numpy as jnp
from jax import lax
from jax.experimental import pallas as pl
from jax.experimental.pallas import tpu as pltpu
from jax.sharding import PartitionSpec as P

AXIS = "mp"
CORES = 2


def norm_body(x_ref, gain_ref, out_ref):
    values = x_ref[...].astype(jnp.float32)
    mean = jnp.mean(values, axis=1, keepdims=True)
    centred = values - mean
    var = jnp.mean(centred * centred, axis=1, keepdims=True)
    out_ref[...] = (centred / jnp.sqrt(var + 1e-05) * gain_ref[...]).astype(jnp.bfloat16)


def normalize(rows, norm_gain):
    count, width = rows.shape
    step = min(16, count)
    return pl.pallas_call(
        norm_body,
        grid=(count // step,),
        in_specs=[
            pl.BlockSpec((step, width), lambda i: (i, 0)),
            pl.BlockSpec((1, width), lambda i: (0, 0)),
        ],
        out_specs=pl.BlockSpec((step, width), lambda i: (i, 0)),
        out_shape=jax.ShapeDtypeStruct(rows.shape, jnp.bfloat16),
        name="norm_rows",
    )(rows, norm_gain.reshape(1, width))


def tie(x, *others):
    return lax.optimization_barrier((x,) + others)[0]


def block(x, w_in, b_in, w_out):
    pre = jnp.dot(x, w_in, preferred_element_type=jnp.float32) + b_in
    hidden = jax.nn.gelu(pre, approximate=True).astype(jnp.bfloat16)
    return jnp.dot(hidden, w_out, preferred_element_type=jnp.float32).astype(jnp.bfloat16)


def grid_of(mesh):
    line = mesh.devices.reshape(-1, mesh.shape[AXIS])[0]
    chips = len(line) // CORES
    coords = [getattr(d, "coords", None) for d in line]
    if coords[0] is None:
        return chips, 1
    wide = len({c[1] for c in coords})
    return (chips // wide, wide) if chips % wide == 0 else (chips, 1)


def solution(mesh):
    long, wide = grid_of(mesh)

    def at(z, y, c):
        return ((z % long) * wide + y % wide) * CORES + c % CORES

    def shift(x, dz, dy, dc):
        pairs = [
            (at(z, y, c), at(z + dz, y + dy, c + dc))
            for z in range(long)
            for y in range(wide)
            for c in range(CORES)
        ]
        return lax.ppermute(x, AXIS, pairs)

    sends = sorted(range(1, long), key=lambda k: min(k, long - k))
    groups = [sends[:1], [0]] + [[k] for k in sends[1:]]

    def local(nodes, norm_gain, w_in, b_in, w_out, b_out):
        rows = nodes.shape[0]
        half = rows * wide
        source = normalize(nodes, norm_gain)
        slots = {0: source}
        for k in sends:
            slots[k] = shift(source, k, 0, 0)

        def spread(x):
            near = [x] + [shift(x, 0, j, 0) for j in range(1, wide)]
            return near, [shift(v, 0, 0, 1) for v in near]

        late = sends[-1]
        near, far, parts, landed = {}, {}, [], []
        for k in [0] + sends[:-1]:
            near[k], far[k] = spread(slots[k])

        def pieces_of(i):
            size = half * len(groups[i])
            found = {}
            for n, k in enumerate(groups[i]):
                for j in range(1, wide):
                    at_row = n * half + j * rows
                    own = parts[i][at_row : at_row + rows].astype(jnp.float32)
                    other = landed[i][size + at_row : size + at_row + rows].astype(jnp.float32)
                    found[k, j] = (own + other).astype(jnp.bfloat16)
            return found

        def total_of(i, k):
            size = half * len(groups[i])
            at_row = groups[i].index(k) * half
            mine = parts[i][at_row : at_row + rows].astype(jnp.float32)
            mine = mine + landed[i][size + at_row : size + at_row + rows].astype(jnp.float32)
            for j in range(1, wide):
                mine = mine + shift(pieces[k, j], 0, -j, 0).astype(jnp.float32)
            return mine

        pieces = {}
        for i, group in enumerate(groups):
            ties = []
            if i == 1:
                slots[late] = tie(slots[late], parts[0])
                near[late], far[late] = spread(slots[late])
                ties.append(slots[late])
            if i >= 1:
                ties.append(parts[i - 1])
            if i >= 2:
                found = pieces_of(i - 2)
                pieces.update(found)
                ties.extend(found.values())
            chunks = [v for k in group for v in near[k]] + [v for k in group for v in far[k]]
            if ties:
                chunks = lax.optimization_barrier(tuple(chunks) + tuple(ties))[: len(chunks)]
            x = jnp.concatenate(chunks, axis=0)
            parts.append(block(x, w_in, b_in, w_out))
            landed.append(shift(parts[i], 0, 0, 1))
        for i in range(max(0, len(groups) - 2), len(groups)):
            pieces.update(pieces_of(i))
        out = nodes.astype(jnp.float32) + b_out
        for i, group in enumerate(groups):
            for k in group:
                mine = total_of(i, k)
                if k:
                    mine = shift(mine.astype(jnp.bfloat16), -k, 0, 0).astype(jnp.float32)
                out = out + mine
        return out.astype(jnp.bfloat16)

    return jax.shard_map(
        local,
        mesh=mesh,
        in_specs=(P(("member", AXIS), None), P(), P(None, AXIS), P(AXIS), P(AXIS, None), P()),
        out_specs=P(("member", AXIS), None),
        check_vma=False,
    )
```

```python
import jax
import jax.numpy as jnp
from jax import lax
from jax.experimental import pallas as pl
from jax.experimental.pallas import tpu as pltpu
from jax.sharding import PartitionSpec as P

AXIS = "mp"
CORES = 2


def norm_body(x_ref, gain_ref, out_ref):
    values = x_ref[...].astype(jnp.float32)
    mean = jnp.mean(values, axis=1, keepdims=True)
    centred = values - mean
    var = jnp.mean(centred * centred, axis=1, keepdims=True)
    out_ref[...] = (centred / jnp.sqrt(var + 1e-05) * gain_ref[...]).astype(jnp.bfloat16)


def normalize(rows, norm_gain):
    count, width = rows.shape
    step = min(16, count)
    return pl.pallas_call(
        norm_body,
        grid=(count // step,),
        in_specs=[
            pl.BlockSpec((step, width), lambda i: (i, 0)),
            pl.BlockSpec((1, width), lambda i: (0, 0)),
        ],
        out_specs=pl.BlockSpec((step, width), lambda i: (i, 0)),
        out_shape=jax.ShapeDtypeStruct(rows.shape, jnp.bfloat16),
        name="norm_rows",
    )(rows, norm_gain.reshape(1, width))


def tie(x, *others):
    return lax.optimization_barrier((x,) + others)[0]


def block(x, w_in, b_in, w_out):
    pre = jnp.dot(x, w_in, preferred_element_type=jnp.float32) + b_in
    hidden = jax.nn.gelu(pre, approximate=True).astype(jnp.bfloat16)
    return jnp.dot(hidden, w_out, preferred_element_type=jnp.float32).astype(jnp.bfloat16)


def grid_of(mesh):
    line = mesh.devices.reshape(-1, mesh.shape[AXIS])[0]
    chips = len(line) // CORES
    coords = [getattr(d, "coords", None) for d in line]
    if coords[0] is None:
        return chips, 1
    wide = len({c[1] for c in coords})
    return (chips // wide, wide) if chips % wide == 0 else (chips, 1)


def solution(mesh):
    long, wide = grid_of(mesh)

    def at(z, y, c):
        return ((z % long) * wide + y % wide) * CORES + c % CORES

    def shift(x, dz, dy, dc):
        pairs = [
            (at(z, y, c), at(z + dz, y + dy, c + dc))
            for z in range(long)
            for y in range(wide)
            for c in range(CORES)
        ]
        return lax.ppermute(x, AXIS, pairs)

    sends = sorted(range(1, long), key=lambda k: min(k, long - k))
    works = sends[:1] + [0] + sends[1:]

    def local(nodes, norm_gain, w_in, b_in, w_out, b_out):
        rows = nodes.shape[0]
        half = rows * wide
        source = normalize(nodes, norm_gain)
        slots = {0: source}
        for k in sends:
            slots[k] = shift(source, k, 0, 0)
        chunks, parts, landed, pieces, totals = {}, {}, {}, {}, {}

        def spread(k):
            near = [slots[k]] + [shift(slots[k], 0, j, 0) for j in range(1, wide)]
            chunks[k] = near + [shift(v, 0, 0, 1) for v in near]

        def own_sum(k, j):
            own = parts[k][j * rows : (j + 1) * rows].astype(jnp.float32)
            return own + landed[k][half + j * rows : half + (j + 1) * rows].astype(jnp.float32)

        def cut(k):
            pieces[k] = [own_sum(k, j).astype(jnp.bfloat16) for j in range(1, wide)]
            return pieces[k]

        def add_up(k):
            mine = own_sum(k, 0)
            for j, piece in enumerate(pieces[k], 1):
                mine = mine + shift(piece, 0, -j, 0).astype(jnp.float32)
            totals[k] = mine.astype(jnp.bfloat16) if k else mine
            return totals[k]

        for k in works[:3]:
            spread(k)
        for i, k in enumerate(works):
            ties = []
            if i >= 1:
                ties.append(parts[works[i - 1]])
                if i + 2 < len(works):
                    ahead = works[i + 2]
                    slots[ahead] = tie(slots[ahead], parts[works[i - 1]])
                    spread(ahead)
                    ties.append(slots[ahead])
            if i >= 2 and works[i - 2]:
                ties.extend(cut(works[i - 2]))
            if i >= 3 and works[i - 3]:
                ties.append(add_up(works[i - 3]))
            held = chunks[k]
            if ties:
                held = lax.optimization_barrier(tuple(held) + tuple(ties))[: len(held)]
            parts[k] = block(jnp.concatenate(held, axis=0), w_in, b_in, w_out)
            landed[k] = shift(parts[k], 0, 0, 1)
        for k in works:
            if k and k not in pieces:
                last = cut(k)
        if last:
            parts[0] = tie(parts[0], last[0])
        cut(0)
        out = nodes.astype(jnp.float32) + b_out
        for k in works:
            if k:
                mine = totals[k] if k in totals else add_up(k)
                out = out + shift(mine, -k, 0, 0).astype(jnp.float32)
        return (out + add_up(0)).astype(jnp.bfloat16)

    return jax.shard_map(
        local,
        mesh=mesh,
        in_specs=(P(("member", AXIS), None), P(), P(None, AXIS), P(AXIS), P(AXIS, None), P()),
        out_specs=P(("member", AXIS), None),
        check_vma=False,
    )
```
